32 devices in a mesh: dp: 2 (over z, core), ep: 16 (over x, y).
Axes of the slice: x: 4, y: 4, z: 1, core: 2. Of those that a mesh axis runs over, the one named last changes fastest.
The devices are a block of a 4x4x4 slice.
Arguments:
- x: bfloat16 [2, 16, 256, 3584], P('dp', 'ep'), parts along dimension 0
- expert: int32 [2, 16, 256, 8], P('dp', 'ep'), parts along dimension 0
- slot: int32 [2, 16, 256, 8], P('dp', 'ep'), parts along dimension 0
- gate: float32 [2, 16, 256, 8], P('dp', 'ep'), parts along dimension 0
- w_gate: bfloat16 [32, 3584, 2560], P('ep')
- w_up: bfloat16 [32, 3584, 2560], P('ep')
- w_down: bfloat16 [32, 2560, 3584], P('ep')
- s_gate: bfloat16 [3584, 20480], replicated
- s_up: bfloat16 [3584, 20480], replicated
- s_down: bfloat16 [20480, 3584], replicated
Outputs:
- y: bfloat16 [2, 16, 256, 3584], P('dp', 'ep'), parts along dimension 0
There are 2 independent parts. The reference program is written for one: setup_inputs(seed, part) draws one part's arguments, and reference() takes and returns one part's arrays. A program takes and returns all parts, laid end to end along the dimension named above; an argument that names none is the same for every part.
All inputs are finite; a program needn't handle non-finite values.
Results may differ from the reference program's by a relative error of at most 0.009.
Values are sent between devices in bfloat16 or wider.
A program may use at most 1.5 GiB of HBM per device.

```python
import jax
import jax.numpy as jnp

MEMBERS = 16
TOKENS = 256
D = 3584
FF = 2560
TOP = 8
EXPERTS = 32
SHARED_FF = 20480
SLOTS = 5 * TOKENS * TOP // (4 * EXPERTS)


def setup_inputs(seed: int = 0, part: int = 0) -> dict:
    own, k1, k2, k3, k4, k5, k6 = jax.random.split(jax.random.key(seed), 7)
    kx, ke, kl, kg = jax.random.split(jax.random.fold_in(own, part), 4)
    devices = (1, MEMBERS)
    place = jax.random.permutation(kl, jnp.arange(EXPERTS, dtype=jnp.uint32))
    slow = ((EXPERTS + (9 * place) % EXPERTS) << ((9 * place) // EXPERTS)) // EXPERTS
    wait = (jax.random.bits(ke, (*devices, TOKENS, EXPERTS), jnp.uint32) >> 10) * slow
    expert = jnp.argsort(wait, axis=-1)[..., :TOP].astype(jnp.int32)
    chosen = jax.nn.one_hot(expert, EXPERTS, dtype=jnp.int32)
    in_line = jnp.cumsum(chosen.reshape(*devices, TOKENS * TOP, EXPERTS), axis=2) - 1
    slot = jnp.sum(in_line.reshape(chosen.shape) * chosen, axis=-1)

    def one(key, rows, columns):
        return (jax.random.normal(key, (rows, columns), jnp.float32) * rows**-0.5).astype(jnp.bfloat16)

    def weights(key, rows, columns):
        return jax.lax.map(lambda k: one(k, rows, columns), jax.random.split(key, EXPERTS))

    return {
        "x": jax.random.normal(kx, (*devices, TOKENS, D), jnp.float32).astype(jnp.bfloat16),
        "expert": expert,
        "slot": slot,
        "gate": jax.nn.softmax(jax.random.normal(kg, expert.shape, jnp.float32)),
        "w_gate": weights(k1, D, FF),
        "w_up": weights(k2, D, FF),
        "w_down": weights(k3, FF, D),
        "s_gate": one(k4, D, SHARED_FF),
        "s_up": one(k5, D, SHARED_FF),
        "s_down": one(k6, SHARED_FF, D),
    }


def einsum(form, a, b):
    return jnp.einsum(form, a.astype(jnp.float32), b.astype(jnp.float32))


def for_all(x, s_gate, s_up, s_down):
    h = jax.nn.silu(einsum("...d,df->...f", x, s_gate)) * einsum("...d,df->...f", x, s_up)
    return einsum("...f,fd->...d", h.astype(jnp.bfloat16), s_down)


def reference(x, expert, slot, gate, w_gate, w_up, w_down, s_gate, s_up, s_down):
    to_expert = jax.nn.one_hot(expert, EXPERTS, dtype=jnp.bfloat16)
    to_slot = jax.nn.one_hot(slot, SLOTS, dtype=jnp.bfloat16)
    weighted = to_expert * gate[..., None].astype(jnp.bfloat16)
    dispatch = einsum("abtke,abtkc->abtec", to_expert, to_slot).astype(jnp.bfloat16)
    combine = einsum("abtke,abtkc->abtec", weighted, to_slot).astype(jnp.bfloat16)
    z = einsum("abtec,abtd->aebcd", dispatch, x).astype(jnp.bfloat16)
    h = jax.nn.silu(einsum("aebcd,edf->aebcf", z, w_gate))
    h = (h * einsum("aebcd,edf->aebcf", z, w_up)).astype(jnp.bfloat16)
    out = einsum("aebcf,efd->aebcd", h, w_down).astype(jnp.bfloat16)
    y = einsum("abtec,aebcd->abtd", combine, out)
    return (y + for_all(x, s_gate, s_up, s_down)).astype(jnp.bfloat16)
```

```python
import functools
import math

import jax
import jax.numpy as jnp
from jax import lax
from jax.experimental import pallas as pl
from jax.experimental.pallas import tpu as pltpu
from jax.sharding import PartitionSpec as P

MESH = pl.DeviceIdType.MESH
F32 = jnp.float32
BF16 = jnp.bfloat16


class Plan:
    def __init__(self, n, t, d, top, experts, ff, sff, ft, col):
        self.n, self.t, self.d, self.top = n, t, d, top
        self.e2 = experts // (n * n)
        self.c = 5 * t * top // (4 * experts)
        self.stride = 1 << (self.c - 1).bit_length()
        self.dh = d // 2
        self.ft, self.col = ft, col
        self.ns, self.nf = sff // ft, ff // ft
        self.cd = n // 2
        self.q = (n // self.cd) * self.e2
        self.nr = self.q * self.nf
        self.steps = self.ns + self.nr
        self.d0 = 12 * self.ns // 40
        self.sb = 25 * self.ns // 40
        self.m = (self.sb + self.nr // 2 + 5, self.sb + self.nr + 9 * self.ns // 40)


def kernel(p, x_hbm, meta, sg, su, sd, wg, wu, wd, y_hbm, xr, zbuf, zsend, ob, ret, part,
           xv, yacc, oacc, hv, zv, cs, ps, mr, gb, ub, db,
           wsem, xsem, p1s, p1r, mts, mtr, ldsem, cpsem, p2s, p2r, zlsem, obsem, p3s, p3r, csem, p4s, p4r):
    n, cc, dh = p.n, p.c, p.dh
    dp, ep = lax.axis_index("dp"), lax.axis_index("ep")
    x, y = ep // n, ep % n
    half = (slice(0, dh), slice(dh, 2 * dh))
    ab = ((x, y), (y, x))

    def mod(v):
        return lax.rem(v + 2 * n, n)

    def at(h, a, b):
        return (dp, a * n + b if h == 0 else b * n + a)

    def place(h, c, b):
        return b if h == 0 else mod(c - b)

    def remote(src, dst, s, r, dev):
        return pltpu.make_async_remote_copy(src, dst, s, r, device_id=dev, device_id_type=MESH)

    def is_r(i):
        return (i >= p.sb) & (i < p.sb + p.nr)

    def start_w(i, which):
        slot = lax.rem(i, 2)
        routed = is_r(i)

        @pl.when((i < p.steps) & jnp.logical_not(routed))
        def _():
            j = jnp.where(i < p.sb, i, i - p.nr)
            o = pl.multiple_of(j * p.ft, p.ft)
            if which == 0:
                pltpu.make_async_copy(sg.at[:, pl.ds(o, p.ft)], gb.at[slot], wsem.at[slot, 0]).start()
                pltpu.make_async_copy(su.at[:, pl.ds(o, p.ft)], ub.at[slot], wsem.at[slot, 1]).start()
            else:
                pltpu.make_async_copy(sd.at[pl.ds(o, p.ft), :], db.at[slot], wsem.at[slot, 2]).start()

        @pl.when(routed)
        def _():
            r = i - p.sb
            e = lax.rem(r // p.nf, p.e2)
            o = pl.multiple_of(lax.rem(r, p.nf) * p.ft, p.ft)
            if which == 0:
                pltpu.make_async_copy(wg.at[e, :, pl.ds(o, p.ft)], gb.at[slot], wsem.at[slot, 0]).start()
                pltpu.make_async_copy(wu.at[e, :, pl.ds(o, p.ft)], ub.at[slot], wsem.at[slot, 1]).start()
            else:
                pltpu.make_async_copy(wd.at[e, pl.ds(o, p.ft), :], db.at[slot], wsem.at[slot, 2]).start()

    def wait_w(slot, which):
        if which == 0:
            pltpu.make_async_copy(sg.at[:, pl.ds(0, p.ft)], gb.at[slot], wsem.at[slot, 0]).wait()
            pltpu.make_async_copy(su.at[:, pl.ds(0, p.ft)], ub.at[slot], wsem.at[slot, 1]).wait()
        else:
            pltpu.make_async_copy(sd.at[pl.ds(0, p.ft), :], db.at[slot], wsem.at[slot, 2]).wait()

    def p1(h, k, sending):
        a, b = ab[h]
        frm = a if sending else mod(a - k)
        dev = at(h, mod(a + k), b)
        return (
            remote(x_hbm.at[:, half[h]], xr.at[h, frm], p1s.at[h, k - 1], p1r.at[h, k - 1], dev),
            remote(meta, mr.at[h, frm], mts.at[h, k - 1], mtr.at[h, k - 1], dev),
        )

    def p2(c, h, k, sending):
        a, b = ab[h]
        to, frm = mod(b + k), (b if sending else mod(b - k))
        return remote(
            zsend.at[c, pl.ds(to * p.e2, p.e2), :, half[h]],
            zbuf.at[:, c * n + place(h, c, frm), :, half[h]],
            p2s.at[c, h, k - 1], p2r.at[c, h, k - 1], at(h, a, to),
        )

    def p3(q, cd, h, k, sending):
        a, b = ab[h]
        c, e = (q // p.e2) * p.cd + cd, lax.rem(q, p.e2)
        to, frm = mod(b + k), (b if sending else mod(b - k))
        return remote(
            ob.at[q, cd * n + place(h, c, to), :, half[h]],
            ret.at[h, frm, c, e],
            p3s.at[c, e, h, k - 1], p3r.at[c, e, h, k - 1], at(h, a, to),
        )

    def p4(c, h):
        a, b = ab[h]
        to = mod(c - b)
        k = mod(to - a)
        return k, remote(ps.at[lax.rem(c, 2), h], part.at[h, a], p4s.at[c, h], p4r.at[h, k], at(h, to, b))

    def rows_of(h, a_src, owner, weighted):
        m = mr[h, a_src]
        out = []
        for e in range(p.e2):
            first = (owner * p.e2 + e) * p.stride
            code = (lax.broadcasted_iota(jnp.int32, (cc, p.t), 0) + first).astype(F32)
            v = jnp.zeros((cc, p.t), F32)
            for k in range(p.top):
                w = m[p.top + k : p.top + k + 1, :] if weighted else 1.0
                v = jnp.where(m[k : k + 1, :] == code, w, v)
            out.append(v.astype(BF16))
        return jnp.concatenate(out, axis=0)

    def load_x(c):
        for h in range(2):
            yield pltpu.make_async_copy(xr.at[h, mod(c - ab[h][1])], ps.at[lax.rem(c, 2), h], ldsem.at[h])

    def staged(c):
        s = lax.rem(c, 2)
        yield pltpu.make_async_copy(zv.at[s], zsend.at[c], cpsem.at[0])
        for h in range(2):
            b = ab[h][1]
            yield pltpu.make_async_copy(
                zv.at[s, pl.ds(b * p.e2, p.e2), :, half[h]],
                zbuf.at[:, c * n + place(h, c, b), :, half[h]],
                cpsem.at[1 + h],
            )

    def dispatch(c):
        s = lax.rem(c, 2)

        def one(b, _):
            for h in range(2):
                a = ab[h][0]
                owner = a * n + b if h == 0 else b * n + a
                rows = rows_of(h, mod(c - ab[h][1]), owner, False)
                for o in range(0, dh, p.col):
                    z = jnp.dot(rows, ps[s, h, :, o : o + p.col], preferred_element_type=F32).astype(BF16)
                    zv[s, pl.ds(b * p.e2, p.e2), :, h * dh + o : h * dh + o + p.col] = z.reshape(p.e2, cc, p.col)
            return 0

        lax.fori_loop(0, n, one, 0)

    def load_z(q):
        chunk, e = q // p.e2, lax.rem(q, p.e2)
        return pltpu.make_async_copy(
            zbuf.at[e, pl.ds(chunk * p.cd * n, p.cd * n)], zv.at[lax.rem(q, 2)], zlsem
        )

    def put_out(q):
        s = lax.rem(q, 2)
        e = lax.rem(q, p.e2)
        yield pltpu.make_async_copy(zv.at[s], ob.at[q], obsem.at[0])
        for cd in range(p.cd):
            c = (q // p.e2) * p.cd + cd
            for h in range(2):
                b = ab[h][1]
                yield pltpu.make_async_copy(
                    zv.at[s, cd * n + place(h, c, b), :, half[h]],
                    ret.at[h, b, c, e],
                    obsem.at[1 + cd * 2 + h],
                )

    def load_ret(c):
        for h in range(2):
            yield [
                pltpu.make_async_copy(ret.at[h, b, c], cs.at[h, pl.ds(b * p.e2, p.e2)], csem.at[h, b])
                for b in range(n)
            ]

    def combine(c):
        for h in range(2):
            a, b = ab[h]
            to = mod(c - b)
            rows = []
            for o in range(n):
                rows.append(rows_of(h, to, a * n + o if h == 0 else o * n + a, True))
            rows = jnp.concatenate(rows, axis=0)
            for o in range(0, dh, p.col):
                v = lax.dot_general(
                    rows, cs[h, :, :, o : o + p.col].reshape(n * p.e2 * cc, p.col),
                    (((0,), (0,)), ((), ())), preferred_element_type=F32,
                )

                @pl.when(to == a)
                def _():
                    yacc[:, h * dh + o : h * dh + o + p.col] += v

                @pl.when(to != a)
                def _():
                    ps[lax.rem(c, 2), h, :, o : o + p.col] = v.astype(BF16)

    def up(src, rows, slot):
        for o in range(0, p.ft, p.col):
            v = src()
            g = jnp.dot(v, gb[slot, :, o : o + p.col], preferred_element_type=F32)
            u = jnp.dot(v, ub[slot, :, o : o + p.col], preferred_element_type=F32)
            hv[:rows, o : o + p.col] = (g * jax.nn.sigmoid(g) * u).astype(BF16)

    def down(acc, rows, slot):
        for o in range(0, p.d, 2 * p.col):
            acc[:, o : o + 2 * p.col] += jnp.dot(
                hv[:rows, :], db[slot, :, o : o + 2 * p.col], preferred_element_type=F32
            )

    big = p.cd * n * cc

    barrier = pltpu.get_barrier_semaphore()
    for h in range(2):
        for k in range(1, n):
            pl.semaphore_signal(barrier, inc=1, device_id=at(h, mod(ab[h][0] + k), ab[h][1]), device_id_type=MESH)
    own = pltpu.make_async_copy(x_hbm, xv, xsem.at[0])
    own.start()
    for i in range(2):
        for which in range(2):
            start_w(jnp.int32(i), which)
    pl.semaphore_wait(barrier, 2 * (n - 1))
    for k in range(1, n):
        for h in range(2):
            for copy in p1(h, k, True):
                copy.start()
    own.wait()
    mine = [pltpu.make_async_copy(xv.at[:, half[h]], xr.at[h, ab[h][0]], xsem.at[h]) for h in range(2)]
    for h in range(2):
        mine[h].start()
        mr[h, ab[h][0]] = meta[...]
    yacc[...] = jnp.zeros_like(yacc)
    oacc[...] = jnp.zeros_like(oacc)
    for h in range(2):
        mine[h].wait()

    def body(i, _):
        slot = lax.rem(i, 2)

        @pl.when(i == p.d0 - 1)
        def _():
            for h in range(2):
                for k in range(1, n):
                    for copy in p1(h, k, False):
                        copy.wait_recv()

        @pl.when((i > p.d0) & (i <= p.d0 + n))
        def _():
            c = i - p.d0 - 1
            for copy in staged(c):
                copy.wait()
            for k in range(1, n):
                for h in range(2):
                    p2(c, h, k, True).start()

        @pl.when((i >= p.d0) & (i < p.d0 + n))
        def _():
            for copy in load_x(i - p.d0):
                copy.wait()

        @pl.when((i >= p.d0 - 1) & (i < p.d0 + n - 1))
        def _():
            for copy in load_x(i - p.d0 + 1):
                copy.start()

        @pl.when((i >= p.d0) & (i < p.d0 + n))
        def _():
            c = i - p.d0
            dispatch(c)
            for copy in staged(c):
                copy.start()

        r = i - p.sb

        @pl.when((r > p.nf) & (r <= p.nr + 1) & (lax.rem(r + p.nf, p.nf) == 1))
        def _():
            q = r // p.nf - 1
            for copy in put_out(q):
                copy.wait()
            for k in range(1, n):
                for cd in range(p.cd):
                    for h in range(2):
                        p3(q, cd, h, k, True).start()

        @pl.when((r > 0) & (r <= p.nr) & (lax.rem(r + p.nf, p.nf) == 0))
        def _():
            q = r // p.nf - 1
            s = lax.rem(q, 2)

            def move(j, _):
                o = pl.multiple_of(j * cc, cc)
                zv[s, j] = oacc[pl.ds(o, cc), :].astype(BF16)
                oacc[pl.ds(o, cc), :] = jnp.zeros((cc, p.d), F32)
                return 0

            lax.fori_loop(0, p.cd * n, move, 0)
            for copy in put_out(q):
                copy.start()

        @pl.when((r >= 0) & (r < p.nr) & (lax.rem(r + p.nf, p.nf) == 0))
        def _():
            load_z(r // p.nf).wait()

        @pl.when((r >= -1) & (r < p.nr - 1) & (lax.rem(r + p.nf, p.nf) == p.nf - 1))
        def _():
            q = (r + 1) // p.nf

            @pl.when(lax.rem(q, p.e2) == 0)
            def _():
                for cd in range(p.cd):
                    for h in range(2):
                        for k in range(1, n):
                            p2((q // p.e2) * p.cd + cd, h, k, False).wait_recv()

            load_z(q).start()

        for g in range(n // p.cd):
            m = p.m[g]

            @pl.when((i > m + 1) & (i <= m + 1 + p.cd))
            def _():
                c = g * p.cd + i - m - 2
                for h in range(2):
                    k, copy = p4(c, h)

                    @pl.when(k != 0)
                    def _():
                        copy.start()

            @pl.when((i > m) & (i <= m + p.cd))
            def _():
                c = g * p.cd + i - m - 1
                for copies in load_ret(c):
                    for copy in copies:
                        copy.wait()
                if g > 0:
                    for h in range(2):
                        k, copy = p4(c - 2, h)

                        @pl.when(k != 0)
                        def _():
                            copy.wait_send()

                combine(c)

            @pl.when((i >= m) & (i < m + p.cd))
            def _():
                cd = i - m
                for e in range(p.e2):
                    for h in range(2):
                        for k in range(1, n):
                            p3(g * p.e2 + e, cd, h, k, False).wait_recv()
                for copies in load_ret(g * p.cd + cd):
                    for copy in copies:
                        copy.start()

        routed = is_r(i)
        zslot = lax.rem(jnp.maximum(r, 0) // p.nf, 2)
        wait_w(slot, 0)

        @pl.when(jnp.logical_not(routed))
        def _():
            up(lambda: xv[...], p.t, slot)

        @pl.when(routed)
        def _():
            up(lambda: zv[zslot].reshape(big, p.d), big, slot)

        start_w(i + 2, 0)
        wait_w(slot, 1)

        @pl.when(jnp.logical_not(routed))
        def _():
            down(yacc, p.t, slot)

        @pl.when(routed)
        def _():
            down(oacc, big, slot)

        start_w(i + 2, 1)
        return 0

    lax.fori_loop(0, p.steps, body, 0)

    for h in range(2):
        for k in range(1, n):
            for copy in p1(h, k, True):
                copy.wait_send()
    for c in range(n):
        for h in range(2):
            for k in range(1, n):
                p2(c, h, k, True).wait_send()
                for e in range(p.e2):
                    p3((c // p.cd) * p.e2 + e, c % p.cd, h, k, True).wait_send()
    for c in range(n - 2, n):
        for h in range(2):
            k, copy = p4(c, h)

            @pl.when(k != 0)
            def _():
                copy.wait_send()

    def arrived(h, k):
        a, b = ab[h]
        return remote(ps.at[0, h], part.at[h, mod(a - k)], p4s.at[0, h], p4r.at[h, k], at(h, mod(a + k), b))

    def fetch(h, k):
        return pltpu.make_async_copy(part.at[h, mod(ab[h][0] - k)], ps.at[lax.rem(k, 2), h], ldsem.at[h])

    for k in range(1, n):
        for h in range(2):
            arrived(h, k).wait_recv()
            fetch(h, k).start()
        for h in range(2):
            fetch(h, k).wait()
            for o in range(0, dh, p.col):
                yacc[:, h * dh + o : h * dh + o + p.col] += ps[k % 2, h, :, o : o + p.col].astype(F32)
    xv[...] = yacc[...].astype(BF16)
    last = pltpu.make_async_copy(xv, y_hbm, xsem.at[0])
    last.start()
    last.wait()


def build(mesh, ft=512, col=256):
    members = mesh.shape["ep"]
    n = math.isqrt(members)

    def step(x, expert, slot, gate, w_gate, w_up, w_down, s_gate, s_up, s_down):
        t, d = x.shape[2:]
        top = expert.shape[3]
        local, _, ff = w_gate.shape
        p = Plan(n, t, d, top, local * members, ff, s_gate.shape[1], ft, col)
        code = jnp.where(slot < p.c, expert * p.stride + slot, -1).astype(F32)
        weight = gate.astype(BF16).astype(F32)
        meta = jnp.concatenate([code[0, 0].T, weight[0, 0].T], axis=0)
        hbm = pl.BlockSpec(memory_space=pl.ANY)
        dma = pltpu.SemaphoreType.DMA
        blocks = p.cd * n
        outs = pl.pallas_call(
            functools.partial(kernel, p),
            name="moe",
            out_shape=(
                jax.ShapeDtypeStruct((t, d), BF16),
                jax.ShapeDtypeStruct((2, n, t, p.dh), BF16),
                jax.ShapeDtypeStruct((p.e2, n * n, p.c, d), BF16),
                jax.ShapeDtypeStruct((n, n * p.e2, p.c, d), BF16),
                jax.ShapeDtypeStruct((p.q, blocks, p.c, d), BF16),
                jax.ShapeDtypeStruct((2, n, n, p.e2, p.c, p.dh), BF16),
                jax.ShapeDtypeStruct((2, n, t, p.dh), BF16),
            ),
            in_specs=[hbm, pl.BlockSpec(memory_space=pltpu.VMEM)] + [hbm] * 6,
            out_specs=(hbm,) * 7,
            scratch_shapes=[
                pltpu.VMEM((t, d), BF16),
                pltpu.VMEM((t, d), F32),
                pltpu.VMEM((blocks * p.c, d), F32),
                pltpu.VMEM((max(t, blocks * p.c), ft), BF16),
                pltpu.VMEM((2, blocks, p.c, d), BF16),
                pltpu.VMEM((2, n * p.e2, p.c, p.dh), BF16),
                pltpu.VMEM((2, 2, t, p.dh), BF16),
                pltpu.VMEM((2, n, 2 * top, t), F32),
                pltpu.VMEM((2, d, ft), BF16),
                pltpu.VMEM((2, d, ft), BF16),
                pltpu.VMEM((2, ft, d), BF16),
                dma((2, 3)),
                dma((2,)),
                dma((2, n - 1)),
                dma((2, n - 1)),
                dma((2, n - 1)),
                dma((2, n - 1)),
                dma((2,)),
                dma((3,)),
                dma((n, 2, n - 1)),
                dma((n, 2, n - 1)),
                dma,
                dma((1 + 2 * p.cd,)),
                dma((n, p.e2, 2, n - 1)),
                dma((n, p.e2, 2, n - 1)),
                dma((2, n)),
                dma((n, 2)),
                dma((2, n)),
            ],
            compiler_params=pltpu.CompilerParams(
                collective_id=0, has_side_effects=True, vmem_limit_bytes=67_000_000
            ),
        )(x[0, 0], meta, s_gate, s_up, s_down, w_gate, w_up, w_down)
        return outs[0][None, None]

    tokens = P("dp", "ep", None, None)
    return jax.shard_map(
        step,
        mesh=mesh,
        in_specs=(tokens,) * 4 + (P("ep", None, None),) * 3 + (P(None, None),) * 3,
        out_specs=tokens,
        check_vma=False,
    )


def solution(mesh):
    return build(mesh)
```

```python
import functools
import math

import jax
import jax.numpy as jnp
from jax import lax
from jax.experimental import pallas as pl
from jax.experimental.pallas import tpu as pltpu
from jax.sharding import PartitionSpec as P

MESH = pl.DeviceIdType.MESH
F32 = jnp.float32
BF16 = jnp.bfloat16


class Plan:
    def __init__(self, n, t, d, top, experts, ff, sff, ft, col):
        self.n, self.t, self.d, self.top = n, t, d, top
        self.e2 = experts // (n * n)
        self.c = 5 * t * top // (4 * experts)
        self.stride = 1 << (self.c - 1).bit_length()
        self.dh = d // 2
        self.ft, self.col = ft, col
        self.edge = d // 4
        self.ns, self.nf = sff // ft, ff // ft
        self.sizes = (1, 2, 1)
        self.ahead = [18, 3, 0]
        self.hop, self.d0 = 7, 10
        self.lag = [[5], [8, 9], [9]]
        self.later = [1, 6, 7]
        self.sum_lag = [2, 6, 6, 4]
        self.tune()

    def tune(self):
        e2, nf = self.e2, self.nf
        self.first = [sum(self.sizes[:g]) for g in range(len(self.sizes))]
        self.start = []
        at = 0
        for ahead in self.ahead:
            self.start.append(at + ahead)
            at += ahead + e2 * nf
        self.q = len(self.sizes) * e2
        self.steps = self.ns + self.q * nf
        self.begin = [self.start[q // e2] + q % e2 * nf for q in range(self.q)]
        self.back = [self.start[g] + e2 * nf + v for g, lags in enumerate(self.lag) for v in lags]
        self.sums = [v + 1 + w for v, w in zip(self.back, self.sum_lag)]
        self.send = [self.d0 + v for v in self.later] + [self.start[0] + e2 * nf + 1]


def among(i, steps):
    hit = i == steps[0]
    for v in steps[1:]:
        hit = hit | (i == v)
    return hit


def count(i, steps):
    total = (i >= steps[0]).astype(jnp.int32)
    for v in steps[1:]:
        total = total + (i >= v).astype(jnp.int32)
    return total


def pick(g, values):
    v = jnp.int32(values[0])
    for j in range(1, len(values)):
        v = jnp.where(g >= j, jnp.int32(values[j]), v)
    return v


def kernel(p, x_hbm, meta, sg, su, sd, wg, wu, wd, y_hbm, xr, zbuf, zsend, ob, ret,
           part, xv, yacc, oacc, hv, zv, cs, ps, pf, fr, wt, mr, gb, ub, db,
           wsem, xsem, p1s, p1r, fws, fwr, mts, mtr, ldsem, cpsem, p2s, p2r, zlsem, obsem, p3s, p3r, csem, p4s, frr, p4r):
    n, cc, dh = p.n, p.c, p.dh
    dp, ep = lax.axis_index("dp"), lax.axis_index("ep")
    x, y = ep // n, ep % n
    half = (slice(0, dh), slice(dh, 2 * dh))
    ab = ((x, y), (y, x))

    def mod(v):
        return lax.rem(v + 2 * n, n)

    def at(h, a, b):
        return (dp, a * n + b if h == 0 else b * n + a)

    def place(h, c, b):
        return b if h == 0 else mod(c - b)

    def remote(src, dst, s, r, dev):
        return pltpu.make_async_remote_copy(src, dst, s, r, device_id=dev, device_id_type=MESH)

    def kind(i):
        g = count(i, p.start) - 1
        r = i - pick(g, p.start)
        routed = (g >= 0) & (r < p.e2 * p.nf)
        passed = jnp.maximum(g, 0) * (p.e2 * p.nf)
        ended = jnp.where(g >= 0, passed + p.e2 * p.nf, 0)
        return routed, g, jnp.where(routed, r, i - ended)

    def start_w(i, which):
        slot = lax.rem(i, 2)
        routed, _, r = kind(i)

        @pl.when((i < p.steps) & jnp.logical_not(routed))
        def _():
            o = pl.multiple_of(r * p.ft, p.ft)
            if which == 0:
                pltpu.make_async_copy(sg.at[:, pl.ds(o, p.ft)], gb.at[slot], wsem.at[slot, 0]).start()
                pltpu.make_async_copy(su.at[:, pl.ds(o, p.ft)], ub.at[slot], wsem.at[slot, 1]).start()
            else:
                pltpu.make_async_copy(sd.at[pl.ds(o, p.ft), :], db.at[slot], wsem.at[slot, 2]).start()

        @pl.when(routed)
        def _():
            e = r // p.nf
            o = pl.multiple_of(lax.rem(r, p.nf) * p.ft, p.ft)
            if which == 0:
                pltpu.make_async_copy(wg.at[e, :, pl.ds(o, p.ft)], gb.at[slot], wsem.at[slot, 0]).start()
                pltpu.make_async_copy(wu.at[e, :, pl.ds(o, p.ft)], ub.at[slot], wsem.at[slot, 1]).start()
            else:
                pltpu.make_async_copy(wd.at[e, pl.ds(o, p.ft), :], db.at[slot], wsem.at[slot, 2]).start()

    def wait_w(slot, which):
        if which == 0:
            pltpu.make_async_copy(sg.at[:, pl.ds(0, p.ft)], gb.at[slot], wsem.at[slot, 0]).wait()
            pltpu.make_async_copy(su.at[:, pl.ds(0, p.ft)], ub.at[slot], wsem.at[slot, 1]).wait()
        else:
            pltpu.make_async_copy(sd.at[pl.ds(0, p.ft), :], db.at[slot], wsem.at[slot, 2]).wait()

    def p1(h, k, sending):
        a, b = ab[h]
        frm = a if sending else mod(a - k)
        return remote(x_hbm.at[:, half[h]], xr.at[h, frm], p1s.at[h, k - 1], p1r.at[h, k - 1], at(h, mod(a + k), b))

    def pass_on(h, k, sending):
        a, b = ab[h]
        frm = mod(a - k) if sending else mod(a - 2 * k)
        rows = pl.ds(0 if k == 1 else p.t // 2, p.t // 2)
        j = 0 if k == 1 else 1
        return remote(xr.at[h, frm, rows], xr.at[h, frm, rows], fws.at[h, j], fwr.at[h, j], at(h, mod(a + k), b))

    def tell(h, k, sending):
        a, b = ab[h]
        frm = a if sending else mod(a - k)
        return remote(meta, mr.at[h, frm], mts.at[h, k - 1], mtr.at[h, k - 1], at(h, mod(a + k), b))

    def p2(c, h, k, sending):
        a, b = ab[h]
        to, frm = mod(b + k), (b if sending else mod(b - k))
        return remote(
            zsend.at[c, pl.ds(to * p.e2, p.e2), :, half[h]],
            zbuf.at[:, c * n + place(h, c, frm), :, half[h]],
            p2s.at[c, h, k - 1], p2r.at[c, h, k - 1], at(h, a, to),
        )

    def p3(c, e, h, k, sending):
        a, b = ab[h]
        to, frm = mod(b + k), (b if sending else mod(b - k))
        return remote(
            ob.at[c, e, place(h, c, to), :, half[h]],
            ret.at[h, frm, c, e],
            p3s.at[c, e, h, k - 1], p3r.at[c, e, h, k - 1], at(h, a, to),
        )

    quarter = (slice(0, dh // 2), slice(dh // 2, dh))

    def away(c, h):
        a, b = ab[h]
        return mod(c - b - a)

    def halfway(c, h, v):
        a, b = ab[h]
        return remote(
            ps.at[lax.rem(c, 2), h, :, quarter[v]], fr.at[h, v], p4s.at[c, h, v], frr.at[h, v],
            at(h, mod(a + 1 - 2 * v), b),
        )

    def home(c, h, side, v):
        a, b = ab[h]
        return remote(
            ps.at[lax.rem(c, 2), h, :, quarter[v]], part.at[h, side, :, quarter[v]],
            p4s.at[c, h, v], p4r.at[h, side, v], at(h, mod(a + 1 - 2 * side), b),
        )

    def rows_of(h, a_src, owner, weighted):
        m = mr[h, a_src]
        out = []
        for e in range(p.e2):
            first = (owner * p.e2 + e) * p.stride
            code = (lax.broadcasted_iota(jnp.int32, (cc, p.t), 0) + first).astype(F32)
            v = jnp.zeros((cc, p.t), F32)
            for k in range(p.top):
                w = m[p.top + k : p.top + k + 1, :] if weighted else 1.0
                v = jnp.where(m[k : k + 1, :] == code, w, v)
            out.append(v)
        return jnp.concatenate(out, axis=0)

    def load_x(c):
        for h in range(2):
            yield pltpu.make_async_copy(xr.at[h, mod(c - ab[h][1])], ps.at[lax.rem(c, 2), h], ldsem.at[h])

    def staged(c):
        s = lax.rem(c, 2)
        yield pltpu.make_async_copy(zv.at[s], zsend.at[c], cpsem.at[0])
        for h in range(2):
            b = ab[h][1]
            yield pltpu.make_async_copy(
                zv.at[s, pl.ds(b * p.e2, p.e2), :, half[h]],
                zbuf.at[:, c * n + place(h, c, b), :, half[h]],
                cpsem.at[1 + h],
            )

    def dispatch(c):
        s = lax.rem(c, 2)

        def one(b, _):
            for h in range(2):
                a = ab[h][0]
                owner = a * n + b if h == 0 else b * n + a
                rows = rows_of(h, mod(c - ab[h][1]), owner, False).astype(BF16)
                for o in range(0, dh, p.col):
                    z = jnp.dot(rows, ps[s, h, :, o : o + p.col], preferred_element_type=F32).astype(BF16)
                    zv[s, pl.ds(b * p.e2, p.e2), :, h * dh + o : h * dh + o + p.col] = z.reshape(p.e2, cc, p.col)
            return 0

        lax.fori_loop(0, n, one, 0)

    def load_z(q):
        g, e = q // p.e2, lax.rem(q, p.e2)
        c = pick(g, p.first)
        for j in range(max(p.sizes)):
            yield j < pick(g, p.sizes), c + j, pltpu.make_async_copy(
                zbuf.at[e, pl.ds((c + j) * n, n)], zv.at[lax.rem(q, 2), pl.ds(j * n, n)], zlsem.at[j]
            )

    def put_out(q):
        s = lax.rem(q, 2)
        g, e = q // p.e2, lax.rem(q, p.e2)
        for j in range(max(p.sizes)):
            c = pick(g, p.first) + j
            copies = [pltpu.make_async_copy(zv.at[s, pl.ds(j * n, n)], ob.at[c, e], obsem.at[j, 0])]
            for h in range(2):
                b = ab[h][1]
                copies.append(
                    pltpu.make_async_copy(
                        zv.at[s, j * n + place(h, c, b), :, half[h]], ret.at[h, b, c, e], obsem.at[j, 1 + h]
                    )
                )
            yield j < pick(g, p.sizes), c, copies

    def load_ret(c):
        for h in range(2):
            for b in range(n):
                yield pltpu.make_async_copy(ret.at[h, b, c], cs.at[h, pl.ds(b * p.e2, p.e2)], csem.at[h, b])

    def combine(c):
        s = lax.rem(c, 2)
        for h in range(2):
            a, b = ab[h]
            to = mod(c - b)
            rows = [rows_of(h, to, a * n + o if h == 0 else o * n + a, True) for o in range(n)]
            wt[h] = jnp.concatenate(rows, axis=0).T.astype(BF16)

            def weighed(o, w=p.col):
                v = cs[h, :, :, o : o + w].reshape(n * p.e2 * cc, w)
                return jnp.dot(wt[h], v, preferred_element_type=F32)

            k = mod(to - a)

            @pl.when(k == 0)
            def _():
                for o in range(0, dh, p.col):
                    yacc[:, h * dh + o : h * dh + o + p.col] += weighed(o)

            @pl.when(k == n // 2)
            def _():
                for v in range(2):
                    for o in range(v * dh // 2, (v + 1) * dh // 2, p.edge):
                        ps[s, h, :, o : o + p.edge] = weighed(o, p.edge).astype(BF16)
                    halfway(c, h, v).start()

            for side in range(2):

                @pl.when(k == (1, n - 1)[side])
                def _():
                    early, late = (1 - side) * dh // 2, side * dh // 2
                    for o in range(early, early + dh // 2, p.edge):
                        ps[s, h, :, o : o + p.edge] = weighed(o, p.edge).astype(BF16)
                    home(c, h, side, 1 - side).start()
                    for o in range(late, late + dh // 2, p.edge):
                        pf[h, :, o - late : o - late + p.edge] = weighed(o, p.edge)

    def add_far(c):
        for h in range(2):
            for side in range(2):

                @pl.when(away(c, h) == (1, n - 1)[side])
                def _():
                    halfway(c, h, side).wait_recv()
                    ps[lax.rem(c, 2), h, :, quarter[side]] = (pf[h] + fr[h, side].astype(F32)).astype(BF16)
                    home(c, h, side, side).start()

    def left(c):
        for h in range(2):

            @pl.when(away(c, h) != 0)
            def _():
                for v in range(2):
                    halfway(c, h, v).wait_send()

    def up(src, rows, slot):
        part_of = min(rows, n * cc) if rows > p.t else rows
        for m in range(0, rows, part_of):
            for o in range(0, p.ft, p.col):
                v = src(m, part_of)
                g = jnp.dot(v, gb[slot, :, o : o + p.col], preferred_element_type=F32)
                u = jnp.dot(v, ub[slot, :, o : o + p.col], preferred_element_type=F32)
                hv[m : m + part_of, o : o + p.col] = (g * jax.nn.sigmoid(g) * u).astype(BF16)

    def down(acc, rows, slot):
        part_of = min(rows, n * cc) if rows > p.t else rows
        for m in range(0, rows, part_of):
            for o in range(0, p.d, 2 * p.col):
                acc[m : m + part_of, o : o + 2 * p.col] += jnp.dot(
                    hv[m : m + part_of, :], db[slot, :, o : o + 2 * p.col], preferred_element_type=F32
                )

    own = pltpu.make_async_copy(x_hbm, xv, xsem.at[0])
    own.start()
    for which in range(2):
        start_w(jnp.int32(0), which)
    barrier = pltpu.get_barrier_semaphore()
    for h in range(2):
        for k in range(1, n):
            pl.semaphore_signal(barrier, inc=1, device_id=at(h, mod(ab[h][0] + k), ab[h][1]), device_id_type=MESH)
    for h in range(2):
        mr[h, ab[h][0]] = meta[...]
    yacc[...] = jnp.zeros_like(yacc)
    pl.semaphore_wait(barrier, 2 * (n - 1))
    near = (1, n - 1)
    for k in near:
        for h in range(2):
            p1(h, k, True).start()
    for k in range(1, n):
        for h in range(2):
            tell(h, k, True).start()
    own.wait()
    for which in range(2):
        start_w(jnp.int32(1), which)
    mine = [pltpu.make_async_copy(xv.at[:, half[h]], xr.at[h, ab[h][0]], xsem.at[h]) for h in range(2)]
    for h in range(2):
        mine[h].start()

    def body(i, _):
        slot = lax.rem(i, 2)

        @pl.when((i >= p.hop) & (i <= p.d0))
        def _():
            @pl.when(i == p.hop)
            def _():
                for k in near:
                    for h in range(2):
                        p1(h, k, False).wait_recv()
                        pass_on(h, k, True).start()

            @pl.when(i == p.d0)
            def _():
                oacc[...] = jnp.zeros_like(oacc)
                for h in range(2):
                    mine[h].wait()
                    for k in near:
                        pass_on(h, k, False).wait_recv()
                    for k in range(1, n):
                        tell(h, k, False).wait_recv()
                for copy in load_x(jnp.int32(0)):
                    copy.start()

        @pl.when((i >= p.begin[0] - 1) & (i <= p.begin[-1] + p.nf))
        def _():
            @pl.when(among(i, [v + p.nf for v in p.begin]))
            def _():
                q = count(i, [v + p.nf for v in p.begin]) - 1
                s = lax.rem(q, 2)

                def move(j, _):
                    o = pl.multiple_of(j * cc, cc)
                    zv[s, j] = oacc[pl.ds(o, cc), :].astype(BF16)
                    oacc[pl.ds(o, cc), :] = jnp.zeros((cc, p.d), F32)
                    return 0

                lax.fori_loop(0, pick(q // p.e2, p.sizes) * n, move, 0)
                for live, c, copies in put_out(q):

                    @pl.when(live)
                    def _():
                        for copy in copies:
                            copy.start()

            @pl.when(among(i, p.begin))
            def _():
                for live, _, copy in load_z(count(i, p.begin) - 1):

                    @pl.when(live)
                    def _():
                        copy.wait()

            @pl.when(among(i, [v - 1 for v in p.begin]))
            def _():
                q = count(i, [v - 1 for v in p.begin]) - 1
                for live, c, copy in load_z(q):

                    @pl.when(live)
                    def _():
                        @pl.when(lax.rem(q, p.e2) == 0)
                        def _():
                            for h in range(2):
                                for k in range(1, n):
                                    p2(c, h, k, False).wait_recv()

                        copy.start()

        @pl.when((i >= p.back[0]) & (i <= p.sums[-1]))
        def _():
            @pl.when(among(i, p.sums))
            def _():
                add_far(count(i, p.sums) - 1)

            @pl.when(among(i, [v + 1 for v in p.back]))
            def _():
                c = count(i, p.back) - 1 - among(i, p.back).astype(jnp.int32)
                for copy in load_ret(c):
                    copy.wait()

                @pl.when(c >= 2)
                def _():
                    left(c - 2)

                combine(c)

            @pl.when(among(i, p.back))
            def _():
                c = count(i, p.back) - 1
                for e in range(p.e2):
                    for h in range(2):
                        for k in range(1, n):
                            p3(c, e, h, k, False).wait_recv()
                for copy in load_ret(c):
                    copy.start()

        routed, g, r = kind(i)
        q = g * p.e2 + r // p.nf
        size = pick(g, p.sizes)
        zslot = lax.rem(jnp.maximum(q, 0), 2)
        wait_w(slot, 0)

        @pl.when(jnp.logical_not(routed))
        def _():
            up(lambda m, r: xv[...], p.t, slot)

        for v in sorted(set(p.sizes)):
            big = v * n * cc

            @pl.when(routed & (size == v))
            def _():
                up(lambda m, r: zv[zslot, m // cc : (m + r) // cc].reshape(r, p.d), big, slot)

        start_w(i + 2, 0)

        @pl.when((i >= p.d0) & (i <= p.send[-1]))
        def _():
            c = i - p.d0

            @pl.when((c > 0) & (c <= n))
            def _():
                for copy in staged(c - 1):
                    copy.wait()

            @pl.when(among(i, p.send))
            def _():
                c = count(i, p.send) - 1
                for k in range(1, n):
                    for h in range(2):
                        p2(c, h, k, True).start()

            @pl.when(c < n)
            def _():
                for copy in load_x(c):
                    copy.wait()

            @pl.when(c < n - 1)
            def _():
                for copy in load_x(c + 1):
                    copy.start()

            @pl.when(c < n)
            def _():
                dispatch(c)
                for copy in staged(c):
                    copy.start()

        @pl.when(among(i, [v + p.nf for v in p.begin]))
        def _():
            q = count(i, [v + p.nf for v in p.begin]) - 1
            for live, c, copies in put_out(q):

                @pl.when(live)
                def _():
                    for copy in copies:
                        copy.wait()
                    for k in range(1, n):
                        for h in range(2):
                            p3(c, lax.rem(q, p.e2), h, k, True).start()

        wait_w(slot, 1)

        @pl.when(jnp.logical_not(routed))
        def _():
            down(yacc, p.t, slot)

        for v in sorted(set(p.sizes)):
            big = v * n * cc

            @pl.when(routed & (size == v))
            def _():
                down(oacc, big, slot)

        start_w(i + 2, 1)
        return 0

    lax.fori_loop(0, p.steps, body, 0)

    for h in range(2):
        for side in range(2):
            for v in range(2):
                home(0, h, side, v).wait_recv()
        for o in range(0, dh, p.col):
            yacc[:, h * dh + o : h * dh + o + p.col] += part[h, 0, :, o : o + p.col].astype(F32) + part[
                h, 1, :, o : o + p.col
            ].astype(F32)
    last = pltpu.make_async_copy(yacc, y_hbm, xsem.at[0])
    last.start()
    for h in range(2):
        for k in near:
            p1(h, k, True).wait_send()
            pass_on(h, k, True).wait_send()
        for k in range(1, n):
            tell(h, k, True).wait_send()
    for c in range(n):
        for h in range(2):
            for k in range(1, n):
                p2(c, h, k, True).wait_send()
                for e in range(p.e2):
                    p3(c, e, h, k, True).wait_send()
    for c in range(n - 2, n):
        left(c)
    last.wait()


def build(mesh, ft=512, col=256):
    members = mesh.shape["ep"]
    n = math.isqrt(members)

    def step(x, expert, slot, gate, w_gate, w_up, w_down, s_gate, s_up, s_down):
        t, d = x.shape[2:]
        top = expert.shape[3]
        local, _, ff = w_gate.shape
        p = Plan(n, t, d, top, local * members, ff, s_gate.shape[1], ft, col)
        code = jnp.where(slot < p.c, expert * p.stride + slot, -1).astype(F32)
        weight = gate.astype(BF16).astype(F32)
        meta = jnp.concatenate([code[0, 0].T, weight[0, 0].T], axis=0)
        hbm = pl.BlockSpec(memory_space=pl.ANY)
        dma = pltpu.SemaphoreType.DMA
        blocks = max(p.sizes) * n
        outs = pl.pallas_call(
            functools.partial(kernel, p),
            name="moe",
            out_shape=(
                jax.ShapeDtypeStruct((t, d), F32),
                jax.ShapeDtypeStruct((2, n, t, p.dh), BF16),
                jax.ShapeDtypeStruct((p.e2, n * n, p.c, d), BF16),
                jax.ShapeDtypeStruct((n, n * p.e2, p.c, d), BF16),
                jax.ShapeDtypeStruct((n, p.e2, n, p.c, d), BF16),
                jax.ShapeDtypeStruct((2, n, n, p.e2, p.c, p.dh), BF16),
            ),
            in_specs=[hbm, pl.BlockSpec(memory_space=pltpu.VMEM)] + [hbm] * 6,
            out_specs=(hbm,) * 6,
            scratch_shapes=[
                pltpu.VMEM((2, 2, t, p.dh), BF16),
                pltpu.VMEM((t, d), BF16),
                pltpu.VMEM((t, d), F32),
                pltpu.VMEM((blocks * p.c, d), F32),
                pltpu.VMEM((max(t, blocks * p.c), ft), BF16),
                pltpu.VMEM((2, max(blocks, n * p.e2), p.c, d), BF16),
                pltpu.VMEM((2, n * p.e2, p.c, p.dh), BF16),
                pltpu.VMEM((2, 2, t, p.dh), BF16),
                pltpu.VMEM((2, t, p.dh // 2), F32),
                pltpu.VMEM((2, 2, t, p.dh // 2), BF16),
                pltpu.VMEM((2, t, n * p.e2 * p.c), BF16),
                pltpu.VMEM((2, n, 2 * top, t), F32),
                pltpu.VMEM((2, d, ft), BF16),
                pltpu.VMEM((2, d, ft), BF16),
                pltpu.VMEM((2, ft, d), BF16),
                dma((2, 3)),
                dma((2,)),
                dma((2, n - 1)),
                dma((2, n - 1)),
                dma((2, 2)),
                dma((2, 2)),
                dma((2, n - 1)),
                dma((2, n - 1)),
                dma((2,)),
                dma((3,)),
                dma((n, 2, n - 1)),
                dma((n, 2, n - 1)),
                dma((max(p.sizes),)),
                dma((max(p.sizes), 3)),
                dma((n, p.e2, 2, n - 1)),
                dma((n, p.e2, 2, n - 1)),
                dma((2, n)),
                dma((n, 2, 2)),
                dma((2, 2)),
                dma((2, 2, 2)),
            ],
            compiler_params=pltpu.CompilerParams(
                collective_id=0, has_side_effects=True, vmem_limit_bytes=67_000_000
            ),
        )(x[0, 0], meta, s_gate, s_up, s_down, w_gate, w_up, w_down)
        return outs[0].astype(BF16)[None, None]

    tokens = P("dp", "ep", None, None)
    return jax.shard_map(
        step,
        mesh=mesh,
        in_specs=(tokens,) * 4 + (P("ep", None, None),) * 3 + (P(None, None),) * 3,
        out_specs=tokens,
        check_vma=False,
    )


def solution(mesh):
    return build(mesh)
```

```python
import functools
import math

import jax
import jax.numpy as jnp
from jax import lax
from jax.experimental import pallas as pl
from jax.experimental.pallas import tpu as pltpu
from jax.sharding import PartitionSpec as P

MESH = pl.DeviceIdType.MESH
F32 = jnp.float32
BF16 = jnp.bfloat16


class Plan:
    def __init__(self, n, t, d, top, experts, ff, sff, ft, col):
        self.n, self.t, self.d, self.top = n, t, d, top
        self.e2 = experts // (n * n)
        self.c = 5 * t * top // (4 * experts)
        self.stride = 1 << (self.c - 1).bit_length()
        self.dh = d // 2
        self.ft, self.col = ft, col
        self.edge = d // 4
        self.ns, self.nf = sff // ft, ff // ft
        self.sizes = (1, 2, 1)
        self.ahead = [20, 3, 0]
        self.hop, self.d0 = 7, 11
        self.lag = [[5], [8, 9], [9]]
        self.later = [1, 6, 7]
        self.sum_lag = [2, 7, 7, 4]
        self.tune()

    def tune(self):
        e2, nf = self.e2, self.nf
        self.first = [sum(self.sizes[:g]) for g in range(len(self.sizes))]
        self.start = []
        at = 0
        for ahead in self.ahead:
            self.start.append(at + ahead)
            at += ahead + e2 * nf
        self.q = len(self.sizes) * e2
        self.steps = self.ns + self.q * nf
        self.begin = [self.start[q // e2] + q % e2 * nf for q in range(self.q)]
        self.back = [self.start[g] + e2 * nf + v for g, lags in enumerate(self.lag) for v in lags]
        self.sums = [v + 1 + w for v, w in zip(self.back, self.sum_lag)]
        self.send = [self.d0 + v for v in self.later] + [self.start[0] + e2 * nf + 1]


def among(i, steps):
    hit = i == steps[0]
    for v in steps[1:]:
        hit = hit | (i == v)
    return hit


def count(i, steps):
    total = (i >= steps[0]).astype(jnp.int32)
    for v in steps[1:]:
        total = total + (i >= v).astype(jnp.int32)
    return total


def pick(g, values):
    v = jnp.int32(values[0])
    for j in range(1, len(values)):
        v = jnp.where(g >= j, jnp.int32(values[j]), v)
    return v


def kernel(p, x_hbm, expert, place_in, gate, sg, su, sd, wg, wu, wd, y_hbm, xr, zbuf, zsend, ob, ret,
           part, meta, xv, yacc, oacc, hv, zv, cs, ps, pf, fr, wt, mr, gb, ub, db,
           wsem, xsem, p1s, p1r, fws, fwr, mts, mtr, ldsem, cpsem, p2s, p2r, zlsem, obsem, p3s, p3r, csem, p4s, frr, p4r):
    n, cc, dh = p.n, p.c, p.dh
    dp, ep = lax.axis_index("dp"), lax.axis_index("ep")
    x, y = ep // n, ep % n
    half = (slice(0, dh), slice(dh, 2 * dh))
    ab = ((x, y), (y, x))

    def mod(v):
        return lax.rem(v + 2 * n, n)

    def at(h, a, b):
        return (dp, a * n + b if h == 0 else b * n + a)

    def place(h, c, b):
        return b if h == 0 else mod(c - b)

    def remote(src, dst, s, r, dev):
        return pltpu.make_async_remote_copy(src, dst, s, r, device_id=dev, device_id_type=MESH)

    def kind(i):
        g = count(i, p.start) - 1
        r = i - pick(g, p.start)
        routed = (g >= 0) & (r < p.e2 * p.nf)
        passed = jnp.maximum(g, 0) * (p.e2 * p.nf)
        ended = jnp.where(g >= 0, passed + p.e2 * p.nf, 0)
        return routed, g, jnp.where(routed, r, i - ended)

    def start_w(i, which):
        slot = lax.rem(i, 2)
        routed, _, r = kind(i)

        @pl.when((i < p.steps) & jnp.logical_not(routed))
        def _():
            o = pl.multiple_of(r * p.ft, p.ft)
            if which == 0:
                pltpu.make_async_copy(sg.at[:, pl.ds(o, p.ft)], gb.at[slot], wsem.at[slot, 0]).start()
                pltpu.make_async_copy(su.at[:, pl.ds(o, p.ft)], ub.at[slot], wsem.at[slot, 1]).start()
            else:
                pltpu.make_async_copy(sd.at[pl.ds(o, p.ft), :], db.at[slot], wsem.at[slot, 2]).start()

        @pl.when(routed)
        def _():
            e = r // p.nf
            o = pl.multiple_of(lax.rem(r, p.nf) * p.ft, p.ft)
            if which == 0:
                pltpu.make_async_copy(wg.at[e, :, pl.ds(o, p.ft)], gb.at[slot], wsem.at[slot, 0]).start()
                pltpu.make_async_copy(wu.at[e, :, pl.ds(o, p.ft)], ub.at[slot], wsem.at[slot, 1]).start()
            else:
                pltpu.make_async_copy(wd.at[e, pl.ds(o, p.ft), :], db.at[slot], wsem.at[slot, 2]).start()

    def wait_w(slot, which):
        if which == 0:
            pltpu.make_async_copy(sg.at[:, pl.ds(0, p.ft)], gb.at[slot], wsem.at[slot, 0]).wait()
            pltpu.make_async_copy(su.at[:, pl.ds(0, p.ft)], ub.at[slot], wsem.at[slot, 1]).wait()
        else:
            pltpu.make_async_copy(sd.at[pl.ds(0, p.ft), :], db.at[slot], wsem.at[slot, 2]).wait()

    def p1(h, k, sending):
        a, b = ab[h]
        frm = a if sending else mod(a - k)
        return remote(x_hbm.at[:, half[h]], xr.at[h, frm], p1s.at[h, k - 1], p1r.at[h, k - 1], at(h, mod(a + k), b))

    def pass_on(h, k, sending):
        a, b = ab[h]
        frm = mod(a - k) if sending else mod(a - 2 * k)
        rows = pl.ds(0 if k == 1 else p.t // 2, p.t // 2)
        j = 0 if k == 1 else 1
        return remote(xr.at[h, frm, rows], xr.at[h, frm, rows], fws.at[h, j], fwr.at[h, j], at(h, mod(a + k), b))

    def tell(h, k, sending):
        a, b = ab[h]
        frm = a if sending else mod(a - k)
        return remote(meta, mr.at[h, frm], mts.at[h, k - 1], mtr.at[h, k - 1], at(h, mod(a + k), b))

    def p2(c, h, k, sending):
        a, b = ab[h]
        to, frm = mod(b + k), (b if sending else mod(b - k))
        return remote(
            zsend.at[c, pl.ds(to * p.e2, p.e2), :, half[h]],
            zbuf.at[:, c * n + place(h, c, frm), :, half[h]],
            p2s.at[c, h, k - 1], p2r.at[c, h, k - 1], at(h, a, to),
        )

    def p3(c, e, h, k, sending):
        a, b = ab[h]
        to, frm = mod(b + k), (b if sending else mod(b - k))
        return remote(
            ob.at[c, e, place(h, c, to), :, half[h]],
            ret.at[h, frm, c, e],
            p3s.at[c, e, h, k - 1], p3r.at[c, e, h, k - 1], at(h, a, to),
        )

    quarter = (slice(0, dh // 2), slice(dh // 2, dh))

    def away(c, h):
        a, b = ab[h]
        return mod(c - b - a)

    def halfway(c, h, v):
        a, b = ab[h]
        return remote(
            ps.at[lax.rem(c, 2), h, :, quarter[v]], fr.at[h, v], p4s.at[c, h, v], frr.at[h, v],
            at(h, mod(a + 1 - 2 * v), b),
        )

    def home(c, h, side, v):
        a, b = ab[h]
        return remote(
            ps.at[lax.rem(c, 2), h, :, quarter[v]], part.at[h, side, :, quarter[v]],
            p4s.at[c, h, v], p4r.at[h, side, v], at(h, mod(a + 1 - 2 * side), b),
        )

    def rows_of(h, a_src, owner, weighted):
        m = mr[h, a_src]
        out = []
        for e in range(p.e2):
            first = (owner * p.e2 + e) * p.stride
            code = (lax.broadcasted_iota(jnp.int32, (cc, p.t), 0) + first).astype(F32)
            v = jnp.zeros((cc, p.t), F32)
            for k in range(p.top):
                w = m[p.top + k : p.top + k + 1, :] if weighted else 1.0
                v = jnp.where(m[k : k + 1, :] == code, w, v)
            out.append(v)
        return jnp.concatenate(out, axis=0)

    def load_x(c):
        for h in range(2):
            yield pltpu.make_async_copy(xr.at[h, mod(c - ab[h][1])], ps.at[lax.rem(c, 2), h], ldsem.at[h])

    def staged(c):
        s = lax.rem(c, 2)
        yield pltpu.make_async_copy(zv.at[s], zsend.at[c], cpsem.at[0])
        for h in range(2):
            b = ab[h][1]
            yield pltpu.make_async_copy(
                zv.at[s, pl.ds(b * p.e2, p.e2), :, half[h]],
                zbuf.at[:, c * n + place(h, c, b), :, half[h]],
                cpsem.at[1 + h],
            )

    def dispatch(c):
        s = lax.rem(c, 2)

        for h in range(2):
            a, b = ab[h]
            rows = [rows_of(h, mod(c - b), a * n + o if h == 0 else o * n + a, False) for o in range(n)]
            rows = jnp.concatenate(rows, axis=0).astype(BF16)
            for o in range(0, dh, p.col):
                z = jnp.dot(rows, ps[s, h, :, o : o + p.col], preferred_element_type=F32).astype(BF16)
                zv[s, : n * p.e2, :, h * dh + o : h * dh + o + p.col] = z.reshape(n * p.e2, cc, p.col)

    def load_z(q):
        g, e = q // p.e2, lax.rem(q, p.e2)
        c = pick(g, p.first)
        for j in range(max(p.sizes)):
            yield j < pick(g, p.sizes), c + j, pltpu.make_async_copy(
                zbuf.at[e, pl.ds((c + j) * n, n)], zv.at[lax.rem(q, 2), pl.ds(j * n, n)], zlsem.at[j]
            )

    def put_out(q):
        s = lax.rem(q, 2)
        g, e = q // p.e2, lax.rem(q, p.e2)
        for j in range(max(p.sizes)):
            c = pick(g, p.first) + j
            copies = [pltpu.make_async_copy(zv.at[s, pl.ds(j * n, n)], ob.at[c, e], obsem.at[j, 0])]
            for h in range(2):
                b = ab[h][1]
                copies.append(
                    pltpu.make_async_copy(
                        zv.at[s, j * n + place(h, c, b), :, half[h]], ret.at[h, b, c, e], obsem.at[j, 1 + h]
                    )
                )
            yield j < pick(g, p.sizes), c, copies

    def load_ret(c):
        for h in range(2):
            for b in range(n):
                yield pltpu.make_async_copy(ret.at[h, b, c], cs.at[h, pl.ds(b * p.e2, p.e2)], csem.at[h, b])

    def combine(c):
        s = lax.rem(c, 2)
        for h in range(2):
            a, b = ab[h]
            to = mod(c - b)
            rows = [rows_of(h, to, a * n + o if h == 0 else o * n + a, True) for o in range(n)]
            wt[h] = jnp.concatenate(rows, axis=0).T.astype(BF16)

            def weighed(o, w=p.col):
                v = cs[h, :, :, o : o + w].reshape(n * p.e2 * cc, w)
                return jnp.dot(wt[h], v, preferred_element_type=F32)

            k = mod(to - a)

            @pl.when(k == 0)
            def _():
                for o in range(0, dh, p.col):
                    yacc[:, h * dh + o : h * dh + o + p.col] += weighed(o)

            @pl.when(k == n // 2)
            def _():
                for v in range(2):
                    for o in range(v * dh // 2, (v + 1) * dh // 2, p.edge):
                        ps[s, h, :, o : o + p.edge] = weighed(o, p.edge).astype(BF16)
                    halfway(c, h, v).start()

            for side in range(2):

                @pl.when(k == (1, n - 1)[side])
                def _():
                    early, late = (1 - side) * dh // 2, side * dh // 2
                    for o in range(early, early + dh // 2, p.edge):
                        ps[s, h, :, o : o + p.edge] = weighed(o, p.edge).astype(BF16)
                    home(c, h, side, 1 - side).start()
                    for o in range(late, late + dh // 2, p.edge):
                        pf[h, :, o - late : o - late + p.edge] = weighed(o, p.edge)

    def add_far(c):
        for h in range(2):
            for side in range(2):

                @pl.when(away(c, h) == (1, n - 1)[side])
                def _():
                    halfway(c, h, side).wait_recv()
                    ps[lax.rem(c, 2), h, :, quarter[side]] = (pf[h] + fr[h, side].astype(F32)).astype(BF16)
                    home(c, h, side, side).start()

    def left(c):
        for h in range(2):

            @pl.when(away(c, h) != 0)
            def _():
                for v in range(2):
                    halfway(c, h, v).wait_send()

    def up(src, rows, slot):
        part_of = min(rows, n * cc) if rows > p.t else rows
        for m in range(0, rows, part_of):
            for o in range(0, p.ft, p.col):
                v = src(m, part_of)
                g = jnp.dot(v, gb[slot, :, o : o + p.col], preferred_element_type=F32)
                u = jnp.dot(v, ub[slot, :, o : o + p.col], preferred_element_type=F32)
                hv[m : m + part_of, o : o + p.col] = (g * jax.nn.sigmoid(g) * u).astype(BF16)

    def down(acc, rows, slot):
        part_of = min(rows, n * cc) if rows > p.t else rows
        for m in range(0, rows, part_of):
            for o in range(0, p.d, 2 * p.col):
                acc[m : m + part_of, o : o + 2 * p.col] += jnp.dot(
                    hv[m : m + part_of, :], db[slot, :, o : o + 2 * p.col], preferred_element_type=F32
                )

    own = pltpu.make_async_copy(x_hbm, xv, xsem.at[0])
    own.start()
    for which in range(2):
        start_w(jnp.int32(0), which)
    barrier = pltpu.get_barrier_semaphore()
    for h in range(2):
        for k in range(1, n):
            pl.semaphore_signal(barrier, inc=1, device_id=at(h, mod(ab[h][0] + k), ab[h][1]), device_id_type=MESH)
    slots = place_in[...]
    meta[: p.top, :] = jnp.where(slots < cc, expert[...] * p.stride + slots, -1).astype(F32)
    meta[p.top :, :] = gate[...].astype(BF16).astype(F32)
    for h in range(2):
        mr[h, ab[h][0]] = meta[...]
    yacc[...] = jnp.zeros_like(yacc)
    pl.semaphore_wait(barrier, 2 * (n - 1))
    near = (1, n - 1)
    for k in near:
        for h in range(2):
            p1(h, k, True).start()
    for k in range(1, n):
        for h in range(2):
            tell(h, k, True).start()
    own.wait()
    for which in range(2):
        start_w(jnp.int32(1), which)
    mine = [pltpu.make_async_copy(xv.at[:, half[h]], xr.at[h, ab[h][0]], xsem.at[h]) for h in range(2)]
    for h in range(2):
        mine[h].start()

    def body(i, _):
        slot = lax.rem(i, 2)

        @pl.when((i >= p.hop) & (i <= p.d0))
        def _():
            @pl.when(i == p.hop)
            def _():
                for k in near:
                    for h in range(2):
                        p1(h, k, False).wait_recv()
                        pass_on(h, k, True).start()

            @pl.when(i == p.d0)
            def _():
                oacc[...] = jnp.zeros_like(oacc)
                for h in range(2):
                    mine[h].wait()
                    for k in near:
                        pass_on(h, k, False).wait_recv()
                    for k in range(1, n):
                        tell(h, k, False).wait_recv()
                for copy in load_x(jnp.int32(0)):
                    copy.start()

        @pl.when((i >= p.begin[0] - 1) & (i <= p.begin[-1] + p.nf))
        def _():
            @pl.when(among(i, [v + p.nf for v in p.begin]))
            def _():
                q = count(i, [v + p.nf for v in p.begin]) - 1
                s = lax.rem(q, 2)

                def move(j, _):
                    o = pl.multiple_of(j * cc, cc)
                    zv[s, j] = oacc[pl.ds(o, cc), :].astype(BF16)
                    oacc[pl.ds(o, cc), :] = jnp.zeros((cc, p.d), F32)
                    return 0

                lax.fori_loop(0, pick(q // p.e2, p.sizes) * n, move, 0)
                for live, c, copies in put_out(q):

                    @pl.when(live)
                    def _():
                        for copy in copies:
                            copy.start()

            @pl.when(among(i, p.begin))
            def _():
                for live, _, copy in load_z(count(i, p.begin) - 1):

                    @pl.when(live)
                    def _():
                        copy.wait()

            @pl.when(among(i, [v - 1 for v in p.begin]))
            def _():
                q = count(i, [v - 1 for v in p.begin]) - 1
                for live, c, copy in load_z(q):

                    @pl.when(live)
                    def _():
                        @pl.when(lax.rem(q, p.e2) == 0)
                        def _():
                            for h in range(2):
                                for k in range(1, n):
                                    p2(c, h, k, False).wait_recv()

                        copy.start()

        @pl.when((i >= p.back[0]) & (i <= p.sums[-1]))
        def _():
            @pl.when(among(i, p.sums))
            def _():
                add_far(count(i, p.sums) - 1)

            @pl.when(among(i, [v + 1 for v in p.back]))
            def _():
                c = count(i, p.back) - 1 - among(i, p.back).astype(jnp.int32)
                for copy in load_ret(c):
                    copy.wait()

                @pl.when(c >= 2)
                def _():
                    left(c - 2)

                combine(c)

            @pl.when(among(i, p.back))
            def _():
                c = count(i, p.back) - 1
                for e in range(p.e2):
                    for h in range(2):
                        for k in range(1, n):
                            p3(c, e, h, k, False).wait_recv()
                for copy in load_ret(c):
                    copy.start()

        routed, g, r = kind(i)
        q = g * p.e2 + r // p.nf
        size = pick(g, p.sizes)
        zslot = lax.rem(jnp.maximum(q, 0), 2)
        wait_w(slot, 0)

        @pl.when(jnp.logical_not(routed))
        def _():
            up(lambda m, r: xv[...], p.t, slot)

        for v in sorted(set(p.sizes)):
            big = v * n * cc

            @pl.when(routed & (size == v))
            def _():
                up(lambda m, r: zv[zslot, m // cc : (m + r) // cc].reshape(r, p.d), big, slot)

        start_w(i + 2, 0)

        @pl.when((i >= p.d0) & (i <= p.send[-1]))
        def _():
            c = i - p.d0

            @pl.when((c > 0) & (c <= n))
            def _():
                for copy in staged(c - 1):
                    copy.wait()

            @pl.when(among(i, p.send))
            def _():
                c = count(i, p.send) - 1
                for k in range(1, n):
                    for h in range(2):
                        p2(c, h, k, True).start()

            @pl.when(c < n)
            def _():
                for copy in load_x(c):
                    copy.wait()

            @pl.when(c < n - 1)
            def _():
                for copy in load_x(c + 1):
                    copy.start()

            @pl.when(c < n)
            def _():
                dispatch(c)
                for copy in staged(c):
                    copy.start()

        @pl.when(among(i, [v + p.nf for v in p.begin]))
        def _():
            q = count(i, [v + p.nf for v in p.begin]) - 1
            for live, c, copies in put_out(q):

                @pl.when(live)
                def _():
                    for copy in copies:
                        copy.wait()
                    for k in range(1, n):
                        for h in range(2):
                            p3(c, lax.rem(q, p.e2), h, k, True).start()

        wait_w(slot, 1)

        @pl.when(jnp.logical_not(routed))
        def _():
            down(yacc, p.t, slot)

        for v in sorted(set(p.sizes)):
            big = v * n * cc

            @pl.when(routed & (size == v))
            def _():
                down(oacc, big, slot)

        start_w(i + 2, 1)
        return 0

    lax.fori_loop(0, p.steps, body, 0)

    for h in range(2):
        for side in range(2):
            for v in range(2):
                home(0, h, side, v).wait_recv()
        for o in range(0, dh, p.col):
            v = part[h, 0, :, o : o + p.col].astype(F32) + part[h, 1, :, o : o + p.col].astype(F32)
            xv[:, h * dh + o : h * dh + o + p.col] = (yacc[:, h * dh + o : h * dh + o + p.col] + v).astype(BF16)
    last = pltpu.make_async_copy(xv, y_hbm, xsem.at[0])
    last.start()
    for h in range(2):
        for k in near:
            p1(h, k, True).wait_send()
            pass_on(h, k, True).wait_send()
        for k in range(1, n):
            tell(h, k, True).wait_send()
    for c in range(n):
        for h in range(2):
            for k in range(1, n):
                p2(c, h, k, True).wait_send()
                for e in range(p.e2):
                    p3(c, e, h, k, True).wait_send()
    for c in range(n - 2, n):
        left(c)
    last.wait()


def build(mesh, ft=512, col=256):
    members = mesh.shape["ep"]
    n = math.isqrt(members)

    def step(x, expert, slot, gate, w_gate, w_up, w_down, s_gate, s_up, s_down):
        t, d = x.shape[2:]
        top = expert.shape[3]
        local, _, ff = w_gate.shape
        p = Plan(n, t, d, top, local * members, ff, s_gate.shape[1], ft, col)
        hbm = pl.BlockSpec(memory_space=pl.ANY)
        dma = pltpu.SemaphoreType.DMA
        blocks = max(p.sizes) * n
        outs = pl.pallas_call(
            functools.partial(kernel, p),
            name="moe",
            out_shape=(
                jax.ShapeDtypeStruct((t, d), BF16),
                jax.ShapeDtypeStruct((2, n, t, p.dh), BF16),
                jax.ShapeDtypeStruct((p.e2, n * n, p.c, d), BF16),
                jax.ShapeDtypeStruct((n, n * p.e2, p.c, d), BF16),
                jax.ShapeDtypeStruct((n, p.e2, n, p.c, d), BF16),
                jax.ShapeDtypeStruct((2, n, n, p.e2, p.c, p.dh), BF16),
            ),
            in_specs=[hbm] + [pl.BlockSpec(memory_space=pltpu.VMEM)] * 3 + [hbm] * 6,
            out_specs=(hbm,) * 6,
            scratch_shapes=[
                pltpu.VMEM((2, 2, t, p.dh), BF16),
                pltpu.VMEM((2 * top, t), F32),
                pltpu.VMEM((t, d), BF16),
                pltpu.VMEM((t, d), F32),
                pltpu.VMEM((blocks * p.c, d), F32),
                pltpu.VMEM((max(t, blocks * p.c), ft), BF16),
                pltpu.VMEM((2, max(blocks, n * p.e2), p.c, d), BF16),
                pltpu.VMEM((2, n * p.e2, p.c, p.dh), BF16),
                pltpu.VMEM((2, 2, t, p.dh), BF16),
                pltpu.VMEM((2, t, p.dh // 2), F32),
                pltpu.VMEM((2, 2, t, p.dh // 2), BF16),
                pltpu.VMEM((2, t, n * p.e2 * p.c), BF16),
                pltpu.VMEM((2, n, 2 * top, t), F32),
                pltpu.VMEM((2, d, ft), BF16),
                pltpu.VMEM((2, d, ft), BF16),
                pltpu.VMEM((2, ft, d), BF16),
                dma((2, 3)),
                dma((2,)),
                dma((2, n - 1)),
                dma((2, n - 1)),
                dma((2, 2)),
                dma((2, 2)),
                dma((2, n - 1)),
                dma((2, n - 1)),
                dma((2,)),
                dma((3,)),
                dma((n, 2, n - 1)),
                dma((n, 2, n - 1)),
                dma((max(p.sizes),)),
                dma((max(p.sizes), 3)),
                dma((n, p.e2, 2, n - 1)),
                dma((n, p.e2, 2, n - 1)),
                dma((2, n)),
                dma((n, 2, 2)),
                dma((2, 2)),
                dma((2, 2, 2)),
            ],
            compiler_params=pltpu.CompilerParams(
                collective_id=0, has_side_effects=True, vmem_limit_bytes=67_000_000
            ),
        )(x[0, 0], expert[0, 0].T, slot[0, 0].T, gate[0, 0].T, s_gate, s_up, s_down, w_gate, w_up, w_down)
        return outs[0][None, None]

    tokens = P("dp", "ep", None, None)
    return jax.shard_map(
        step,
        mesh=mesh,
        in_specs=(tokens,) * 4 + (P("ep", None, None),) * 3 + (P(None, None),) * 3,
        out_specs=tokens,
        check_vma=False,
    )


def solution(mesh):
    return build(mesh)
```

```python
import functools
import math

import jax
import jax.numpy as jnp
from jax import lax
from jax.experimental import pallas as pl
from jax.experimental.pallas import tpu as pltpu
from jax.sharding import PartitionSpec as P

MESH = pl.DeviceIdType.MESH
F32 = jnp.float32
BF16 = jnp.bfloat16


class Plan:
    def __init__(self, n, t, d, top, experts, ff, sff, ft, col):
        self.n, self.t, self.d, self.top = n, t, d, top
        self.e2 = experts // (n * n)
        self.c = 5 * t * top // (4 * experts)
        self.stride = 1 << (self.c - 1).bit_length()
        self.dh = d // 2
        self.ft, self.col = ft, col
        self.cut = -(-self.dh // (2 * col)) * col
        self.ns, self.nf = sff // ft, ff // ft
        self.sizes = (1, 2, 1)
        self.ahead = [20, 3, 0]
        self.hop, self.d0 = 7, 11
        self.lag = [[5], [8, 9], [9]]
        self.later = [1, 6, 7]
        self.sum_lag = [4, 8, 8, 3]
        self.tune()

    def tune(self):
        e2, nf = self.e2, self.nf
        self.first = [sum(self.sizes[:g]) for g in range(len(self.sizes))]
        self.start = []
        at = 0
        for ahead in self.ahead:
            self.start.append(at + ahead)
            at += ahead + e2 * nf
        self.q = len(self.sizes) * e2
        self.steps = self.ns + self.q * nf
        self.begin = [self.start[q // e2] + q % e2 * nf for q in range(self.q)]
        self.back = [self.start[g] + e2 * nf + v for g, lags in enumerate(self.lag) for v in lags]
        self.sums = [v + 1 + w for v, w in zip(self.back, self.sum_lag)]
        self.send = [self.d0 + v for v in self.later] + [self.start[0] + e2 * nf + 1]


def among(i, steps):
    hit = i == steps[0]
    for v in steps[1:]:
        hit = hit | (i == v)
    return hit


def count(i, steps):
    total = (i >= steps[0]).astype(jnp.int32)
    for v in steps[1:]:
        total = total + (i >= v).astype(jnp.int32)
    return total


def pick(g, values):
    v = jnp.int32(values[0])
    for j in range(1, len(values)):
        v = jnp.where(g >= j, jnp.int32(values[j]), v)
    return v


def kernel(p, x_hbm, expert, place_in, gate, sg, su, sd, wg, wu, wd, y_hbm, xr, zbuf, zsend, ob, ret,
           part, meta, xv, yacc, oacc, hv, zv, cs, ps, pf, fr, wt, mr, gb, ub, db,
           wsem, xsem, p1s, p1r, fws, fwr, mts, mtr, ldsem, cpsem, p2s, p2r, zlsem, obsem, p3s, p3r, csem, p4s, frr, p4r):
    n, cc, dh = p.n, p.c, p.dh
    dp, ep = lax.axis_index("dp"), lax.axis_index("ep")
    x, y = ep // n, ep % n
    half = (slice(0, dh), slice(dh, 2 * dh))
    ab = ((x, y), (y, x))

    def mod(v):
        return lax.rem(v + 2 * n, n)

    def at(h, a, b):
        return (dp, a * n + b if h == 0 else b * n + a)

    def place(h, c, b):
        return b if h == 0 else mod(c - b)

    def remote(src, dst, s, r, dev):
        return pltpu.make_async_remote_copy(src, dst, s, r, device_id=dev, device_id_type=MESH)

    def kind(i):
        g = count(i, p.start) - 1
        r = i - pick(g, p.start)
        routed = (g >= 0) & (r < p.e2 * p.nf)
        passed = jnp.maximum(g, 0) * (p.e2 * p.nf)
        ended = jnp.where(g >= 0, passed + p.e2 * p.nf, 0)
        return routed, g, jnp.where(routed, r, i - ended)

    def start_w(i, which):
        slot = lax.rem(i, 2)
        routed, _, r = kind(i)

        @pl.when((i < p.steps) & jnp.logical_not(routed))
        def _():
            o = pl.multiple_of(r * p.ft, p.ft)
            if which == 0:
                pltpu.make_async_copy(sg.at[:, pl.ds(o, p.ft)], gb.at[slot], wsem.at[slot, 0]).start()
                pltpu.make_async_copy(su.at[:, pl.ds(o, p.ft)], ub.at[slot], wsem.at[slot, 1]).start()
            else:
                pltpu.make_async_copy(sd.at[pl.ds(o, p.ft), :], db.at[slot], wsem.at[slot, 2]).start()

        @pl.when(routed)
        def _():
            e = r // p.nf
            o = pl.multiple_of(lax.rem(r, p.nf) * p.ft, p.ft)
            if which == 0:
                pltpu.make_async_copy(wg.at[e, :, pl.ds(o, p.ft)], gb.at[slot], wsem.at[slot, 0]).start()
                pltpu.make_async_copy(wu.at[e, :, pl.ds(o, p.ft)], ub.at[slot], wsem.at[slot, 1]).start()
            else:
                pltpu.make_async_copy(wd.at[e, pl.ds(o, p.ft), :], db.at[slot], wsem.at[slot, 2]).start()

    def wait_w(slot, which):
        if which == 0:
            pltpu.make_async_copy(sg.at[:, pl.ds(0, p.ft)], gb.at[slot], wsem.at[slot, 0]).wait()
            pltpu.make_async_copy(su.at[:, pl.ds(0, p.ft)], ub.at[slot], wsem.at[slot, 1]).wait()
        else:
            pltpu.make_async_copy(sd.at[pl.ds(0, p.ft), :], db.at[slot], wsem.at[slot, 2]).wait()

    def p1(h, k, sending):
        a, b = ab[h]
        frm = a if sending else mod(a - k)
        return remote(x_hbm.at[:, half[h]], xr.at[h, frm], p1s.at[h, k - 1], p1r.at[h, k - 1], at(h, mod(a + k), b))

    def pass_on(h, k, sending):
        a, b = ab[h]
        frm = mod(a - k) if sending else mod(a - 2 * k)
        rows = pl.ds(0 if k == 1 else p.t // 2, p.t // 2)
        j = 0 if k == 1 else 1
        return remote(xr.at[h, frm, rows], xr.at[h, frm, rows], fws.at[h, j], fwr.at[h, j], at(h, mod(a + k), b))

    def tell(h, k, sending):
        a, b = ab[h]
        frm = a if sending else mod(a - k)
        return remote(meta, mr.at[h, frm], mts.at[h, k - 1], mtr.at[h, k - 1], at(h, mod(a + k), b))

    def p2(c, h, k, sending):
        a, b = ab[h]
        to, frm = mod(b + k), (b if sending else mod(b - k))
        return remote(
            zsend.at[c, pl.ds(to * p.e2, p.e2), :, half[h]],
            zbuf.at[:, c * n + place(h, c, frm), :, half[h]],
            p2s.at[c, h, k - 1], p2r.at[c, h, k - 1], at(h, a, to),
        )

    def p3(c, e, h, k, sending):
        a, b = ab[h]
        to, frm = mod(b + k), (b if sending else mod(b - k))
        return remote(
            ob.at[c, e, place(h, c, to), :, half[h]],
            ret.at[h, frm, c, e],
            p3s.at[c, e, h, k - 1], p3r.at[c, e, h, k - 1], at(h, a, to),
        )

    quarter = (slice(0, p.cut), slice(p.cut, dh))
    wide = (p.cut, dh - p.cut)

    def away(c, h):
        a, b = ab[h]
        return mod(c - b - a)

    def halfway(c, h, v):
        a, b = ab[h]
        return remote(
            ps.at[lax.rem(c, 2), h, :, quarter[v]], fr.at[h, v, :, : wide[v]], p4s.at[c, h, v], frr.at[h, v],
            at(h, mod(a + 1 - 2 * v), b),
        )

    def home(c, h, side, v):
        a, b = ab[h]
        return remote(
            ps.at[lax.rem(c, 2), h, :, quarter[v]], part.at[h, side, :, quarter[v]],
            p4s.at[c, h, v], p4r.at[h, side, v], at(h, mod(a + 1 - 2 * side), b),
        )

    def rows_of(h, a_src, owner, weighted):
        m = mr[h, a_src]
        out = []
        for e in range(p.e2):
            first = (owner * p.e2 + e) * p.stride
            code = (lax.broadcasted_iota(jnp.int32, (cc, p.t), 0) + first).astype(F32)
            v = jnp.zeros((cc, p.t), F32)
            for k in range(p.top):
                w = m[p.top + k : p.top + k + 1, :] if weighted else 1.0
                v = jnp.where(m[k : k + 1, :] == code, w, v)
            out.append(v)
        return jnp.concatenate(out, axis=0)

    def load_x(c):
        for h in range(2):
            yield pltpu.make_async_copy(xr.at[h, mod(c - ab[h][1])], ps.at[lax.rem(c, 2), h], ldsem.at[h])

    def staged(c):
        s = lax.rem(c, 2)
        yield pltpu.make_async_copy(zv.at[s], zsend.at[c], cpsem.at[0])
        for h in range(2):
            b = ab[h][1]
            yield pltpu.make_async_copy(
                zv.at[s, pl.ds(b * p.e2, p.e2), :, half[h]],
                zbuf.at[:, c * n + place(h, c, b), :, half[h]],
                cpsem.at[1 + h],
            )

    def dispatch(c):
        s = lax.rem(c, 2)

        for h in range(2):
            a, b = ab[h]
            rows = [rows_of(h, mod(c - b), a * n + o if h == 0 else o * n + a, False) for o in range(n)]
            rows = jnp.concatenate(rows, axis=0).astype(BF16)
            for o in range(0, dh, p.col):
                z = jnp.dot(rows, ps[s, h, :, o : o + p.col], preferred_element_type=F32).astype(BF16)
                zv[s, : n * p.e2, :, h * dh + o : h * dh + o + p.col] = z.reshape(n * p.e2, cc, p.col)

    def load_z(q):
        g, e = q // p.e2, lax.rem(q, p.e2)
        c = pick(g, p.first)
        for j in range(max(p.sizes)):
            yield j < pick(g, p.sizes), c + j, pltpu.make_async_copy(
                zbuf.at[e, pl.ds((c + j) * n, n)], zv.at[lax.rem(q, 2), pl.ds(j * n, n)], zlsem.at[j]
            )

    def put_out(q):
        s = lax.rem(q, 2)
        g, e = q // p.e2, lax.rem(q, p.e2)
        for j in range(max(p.sizes)):
            c = pick(g, p.first) + j
            copies = [pltpu.make_async_copy(zv.at[s, pl.ds(j * n, n)], ob.at[c, e], obsem.at[j, 0])]
            for h in range(2):
                b = ab[h][1]
                copies.append(
                    pltpu.make_async_copy(
                        zv.at[s, j * n + place(h, c, b), :, half[h]], ret.at[h, b, c, e], obsem.at[j, 1 + h]
                    )
                )
            yield j < pick(g, p.sizes), c, copies

    def load_ret(c):
        for h in range(2):
            for b in range(n):
                yield pltpu.make_async_copy(ret.at[h, b, c], cs.at[h, pl.ds(b * p.e2, p.e2)], csem.at[h, b])

    def combine(c):
        s = lax.rem(c, 2)
        for h in range(2):
            a, b = ab[h]
            to = mod(c - b)
            rows = [rows_of(h, to, a * n + o if h == 0 else o * n + a, True) for o in range(n)]
            wt[h] = jnp.concatenate(rows, axis=0).astype(BF16).T

            def weighed(o):
                v = cs[h, :, :, o : o + p.col].reshape(n * p.e2 * cc, p.col)
                return jnp.dot(wt[h], v, preferred_element_type=F32)

            k = mod(to - a)

            @pl.when(k == 0)
            def _():
                for o in range(0, dh, p.col):
                    yacc[:, h * dh + o : h * dh + o + p.col] += weighed(o)

            @pl.when(k == n // 2)
            def _():
                for v in range(2):
                    for o in range(quarter[v].start, quarter[v].stop, p.col):
                        ps[s, h, :, o : o + p.col] = weighed(o).astype(BF16)
                    halfway(c, h, v).start()

            for side in range(2):

                @pl.when(k == (1, n - 1)[side])
                def _():
                    early, late = quarter[1 - side], quarter[side]
                    for o in range(early.start, early.stop, p.col):
                        ps[s, h, :, o : o + p.col] = weighed(o).astype(BF16)
                    home(c, h, side, 1 - side).start()
                    for o in range(late.start, late.stop, p.col):
                        pf[h, :, o - late.start : o - late.start + p.col] = weighed(o)

    def add_far(c):
        for h in range(2):
            for side in range(2):

                @pl.when(away(c, h) == (1, n - 1)[side])
                def _():
                    halfway(c, h, side).wait_recv()
                    v = pf[h, :, : wide[side]] + fr[h, side, :, : wide[side]].astype(F32)
                    ps[lax.rem(c, 2), h, :, quarter[side]] = v.astype(BF16)
                    home(c, h, side, side).start()

    def left(c):
        for h in range(2):

            @pl.when(away(c, h) != 0)
            def _():
                for v in range(2):
                    halfway(c, h, v).wait_send()

    def up(src, rows, slot):
        part_of = min(rows, n * cc) if rows > p.t else rows
        for m in range(0, rows, part_of):
            for o in range(0, p.ft, p.col):
                v = src(m, part_of)
                g = jnp.dot(v, gb[slot, :, o : o + p.col], preferred_element_type=F32)
                u = jnp.dot(v, ub[slot, :, o : o + p.col], preferred_element_type=F32)
                hv[m : m + part_of, o : o + p.col] = (g * jax.nn.sigmoid(g) * u).astype(BF16)

    def down(acc, rows, slot):
        part_of = min(rows, n * cc) if rows > p.t else rows
        for m in range(0, rows, part_of):
            for o in range(0, p.d, 2 * p.col):
                acc[m : m + part_of, o : o + 2 * p.col] += jnp.dot(
                    hv[m : m + part_of, :], db[slot, :, o : o + 2 * p.col], preferred_element_type=F32
                )

    own = pltpu.make_async_copy(x_hbm, xv, xsem.at[0])
    own.start()
    for which in range(2):
        start_w(jnp.int32(0), which)
    barrier = pltpu.get_barrier_semaphore()
    for h in range(2):
        for k in range(1, n):
            pl.semaphore_signal(barrier, inc=1, device_id=at(h, mod(ab[h][0] + k), ab[h][1]), device_id_type=MESH)
    slots = place_in[...]
    meta[: p.top, :] = jnp.where(slots < cc, expert[...] * p.stride + slots, -1).astype(F32)
    meta[p.top :, :] = gate[...].astype(BF16).astype(F32)
    for h in range(2):
        mr[h, ab[h][0]] = meta[...]
    yacc[...] = jnp.zeros_like(yacc)
    pl.semaphore_wait(barrier, 2 * (n - 1))
    near = (1, n - 1)
    for k in near:
        for h in range(2):
            p1(h, k, True).start()
    for k in range(1, n):
        for h in range(2):
            tell(h, k, True).start()
    own.wait()
    for which in range(2):
        start_w(jnp.int32(1), which)
    mine = [pltpu.make_async_copy(xv.at[:, half[h]], xr.at[h, ab[h][0]], xsem.at[h]) for h in range(2)]
    for h in range(2):
        mine[h].start()

    def body(i, _):
        slot = lax.rem(i, 2)

        @pl.when((i >= p.hop) & (i <= p.d0))
        def _():
            @pl.when(i == p.hop)
            def _():
                for k in near:
                    for h in range(2):
                        p1(h, k, False).wait_recv()
                        pass_on(h, k, True).start()

            @pl.when(i == p.d0)
            def _():
                oacc[...] = jnp.zeros_like(oacc)
                for h in range(2):
                    mine[h].wait()
                    for k in near:
                        pass_on(h, k, False).wait_recv()
                    for k in range(1, n):
                        tell(h, k, False).wait_recv()
                for copy in load_x(jnp.int32(0)):
                    copy.start()

        @pl.when((i >= p.begin[0] - 1) & (i <= p.begin[-1] + p.nf))
        def _():
            @pl.when(among(i, [v + p.nf for v in p.begin]))
            def _():
                q = count(i, [v + p.nf for v in p.begin]) - 1
                s = lax.rem(q, 2)

                def move(j, _):
                    o = pl.multiple_of(j * cc, cc)
                    zv[s, j] = oacc[pl.ds(o, cc), :].astype(BF16)
                    oacc[pl.ds(o, cc), :] = jnp.zeros((cc, p.d), F32)
                    return 0

                lax.fori_loop(0, pick(q // p.e2, p.sizes) * n, move, 0)
                for live, c, copies in put_out(q):

                    @pl.when(live)
                    def _():
                        for copy in copies:
                            copy.start()

            @pl.when(among(i, p.begin))
            def _():
                for live, _, copy in load_z(count(i, p.begin) - 1):

                    @pl.when(live)
                    def _():
                        copy.wait()

            @pl.when(among(i, [v - 1 for v in p.begin]))
            def _():
                q = count(i, [v - 1 for v in p.begin]) - 1
                for live, c, copy in load_z(q):

                    @pl.when(live)
                    def _():
                        @pl.when(lax.rem(q, p.e2) == 0)
                        def _():
                            for h in range(2):
                                for k in range(1, n):
                                    p2(c, h, k, False).wait_recv()

                        copy.start()

        @pl.when((i >= p.back[0]) & (i <= p.sums[-1]))
        def _():
            @pl.when(among(i, p.sums))
            def _():
                add_far(count(i, p.sums) - 1)

            @pl.when(among(i, [v + 1 for v in p.back]))
            def _():
                c = count(i, p.back) - 1 - among(i, p.back).astype(jnp.int32)
                for copy in load_ret(c):
                    copy.wait()

                @pl.when(c >= 2)
                def _():
                    left(c - 2)

                combine(c)

            @pl.when(among(i, p.back))
            def _():
                c = count(i, p.back) - 1
                for e in range(p.e2):
                    for h in range(2):
                        for k in range(1, n):
                            p3(c, e, h, k, False).wait_recv()
                for copy in load_ret(c):
                    copy.start()

        routed, g, r = kind(i)
        q = g * p.e2 + r // p.nf
        size = pick(g, p.sizes)
        zslot = lax.rem(jnp.maximum(q, 0), 2)
        wait_w(slot, 0)

        @pl.when(jnp.logical_not(routed))
        def _():
            up(lambda m, r: xv[...], p.t, slot)

        for v in sorted(set(p.sizes)):
            big = v * n * cc

            @pl.when(routed & (size == v))
            def _():
                up(lambda m, r: zv[zslot, m // cc : (m + r) // cc].reshape(r, p.d), big, slot)

        start_w(i + 2, 0)

        @pl.when((i >= p.d0) & (i <= p.send[-1]))
        def _():
            c = i - p.d0

            @pl.when((c > 0) & (c <= n))
            def _():
                for copy in staged(c - 1):
                    copy.wait()

            @pl.when(among(i, p.send))
            def _():
                c = count(i, p.send) - 1
                for k in range(1, n):
                    for h in range(2):
                        p2(c, h, k, True).start()

            @pl.when(c < n)
            def _():
                for copy in load_x(c):
                    copy.wait()

            @pl.when(c < n - 1)
            def _():
                for copy in load_x(c + 1):
                    copy.start()

            @pl.when(c < n)
            def _():
                dispatch(c)
                for copy in staged(c):
                    copy.start()

        @pl.when(among(i, [v + p.nf for v in p.begin]))
        def _():
            q = count(i, [v + p.nf for v in p.begin]) - 1
            for live, c, copies in put_out(q):

                @pl.when(live)
                def _():
                    for copy in copies:
                        copy.wait()
                    for k in range(1, n):
                        for h in range(2):
                            p3(c, lax.rem(q, p.e2), h, k, True).start()

        wait_w(slot, 1)

        @pl.when(jnp.logical_not(routed))
        def _():
            down(yacc, p.t, slot)

        for v in sorted(set(p.sizes)):
            big = v * n * cc

            @pl.when(routed & (size == v))
            def _():
                down(oacc, big, slot)

        start_w(i + 2, 1)
        return 0

    lax.fori_loop(0, p.steps, body, 0)

    for h in range(2):
        for side in range(2):
            for v in range(2):
                home(0, h, side, v).wait_recv()
        for o in range(0, dh, p.col):
            v = part[h, 0, :, o : o + p.col].astype(F32) + part[h, 1, :, o : o + p.col].astype(F32)
            xv[:, h * dh + o : h * dh + o + p.col] = (yacc[:, h * dh + o : h * dh + o + p.col] + v).astype(BF16)
        pltpu.make_async_copy(xv.at[:, half[h]], y_hbm.at[:, half[h]], xsem.at[h]).start()
    for h in range(2):
        for k in near:
            p1(h, k, True).wait_send()
            pass_on(h, k, True).wait_send()
        for k in range(1, n):
            tell(h, k, True).wait_send()
    for c in range(n):
        for h in range(2):
            for k in range(1, n):
                p2(c, h, k, True).wait_send()
                for e in range(p.e2):
                    p3(c, e, h, k, True).wait_send()
    for c in range(n - 2, n):
        left(c)
    for h in range(2):
        pltpu.make_async_copy(xv.at[:, half[h]], y_hbm.at[:, half[h]], xsem.at[h]).wait()


def build(mesh, ft=512, col=256):
    members = mesh.shape["ep"]
    n = math.isqrt(members)

    def step(x, expert, slot, gate, w_gate, w_up, w_down, s_gate, s_up, s_down):
        t, d = x.shape[2:]
        top = expert.shape[3]
        local, _, ff = w_gate.shape
        p = Plan(n, t, d, top, local * members, ff, s_gate.shape[1], ft, col)
        hbm = pl.BlockSpec(memory_space=pl.ANY)
        dma = pltpu.SemaphoreType.DMA
        blocks = max(p.sizes) * n
        outs = pl.pallas_call(
            functools.partial(kernel, p),
            name="moe",
            out_shape=(
                jax.ShapeDtypeStruct((t, d), BF16),
                jax.ShapeDtypeStruct((2, n, t, p.dh), BF16),
                jax.ShapeDtypeStruct((p.e2, n * n, p.c, d), BF16),
                jax.ShapeDtypeStruct((n, n * p.e2, p.c, d), BF16),
                jax.ShapeDtypeStruct((n, p.e2, n, p.c, d), BF16),
                jax.ShapeDtypeStruct((2, n, n, p.e2, p.c, p.dh), BF16),
            ),
            in_specs=[hbm] + [pl.BlockSpec(memory_space=pltpu.VMEM)] * 3 + [hbm] * 6,
            out_specs=(hbm,) * 6,
            scratch_shapes=[
                pltpu.VMEM((2, 2, t, p.dh), BF16),
                pltpu.VMEM((2 * top, t), F32),
                pltpu.VMEM((t, d), BF16),
                pltpu.VMEM((t, d), F32),
                pltpu.VMEM((blocks * p.c, d), F32),
                pltpu.VMEM((max(t, blocks * p.c), ft), BF16),
                pltpu.VMEM((2, max(blocks, n * p.e2), p.c, d), BF16),
                pltpu.VMEM((2, n * p.e2, p.c, p.dh), BF16),
                pltpu.VMEM((2, 2, t, p.dh), BF16),
                pltpu.VMEM((2, t, p.cut), F32),
                pltpu.VMEM((2, 2, t, p.cut), BF16),
                pltpu.VMEM((2, t, n * p.e2 * p.c), BF16),
                pltpu.VMEM((2, n, 2 * top, t), F32),
                pltpu.VMEM((2, d, ft), BF16),
                pltpu.VMEM((2, d, ft), BF16),
                pltpu.VMEM((2, ft, d), BF16),
                dma((2, 3)),
                dma((2,)),
                dma((2, n - 1)),
                dma((2, n - 1)),
                dma((2, 2)),
                dma((2, 2)),
                dma((2, n - 1)),
                dma((2, n - 1)),
                dma((2,)),
                dma((3,)),
                dma((n, 2, n - 1)),
                dma((n, 2, n - 1)),
                dma((max(p.sizes),)),
                dma((max(p.sizes), 3)),
                dma((n, p.e2, 2, n - 1)),
                dma((n, p.e2, 2, n - 1)),
                dma((2, n)),
                dma((n, 2, 2)),
                dma((2, 2)),
                dma((2, 2, 2)),
            ],
            compiler_params=pltpu.CompilerParams(
                collective_id=0, has_side_effects=True, vmem_limit_bytes=67_000_000
            ),
        )(x[0, 0], expert[0, 0].T, slot[0, 0].T, gate[0, 0].T, s_gate, s_up, s_down, w_gate, w_up, w_down)
        return outs[0][None, None]

    tokens = P("dp", "ep", None, None)
    return jax.shard_map(
        step,
        mesh=mesh,
        in_specs=(tokens,) * 4 + (P("ep", None, None),) * 3 + (P(None, None),) * 3,
        out_specs=tokens,
        check_vma=False,
    )


def solution(mesh):
    return build(mesh)
```
